32 devices in a mesh: row: 16 (over z, y, x), col: 2 (over core).
Axes of the slice: x: 2, y: 2, z: 4, core: 2. Of those that a mesh axis runs over, the one named last changes fastest.
Arguments:
- orbitals: float32 [3072, 512], P(('row', 'col')), may hold values from -6 to 6
- coulomb: float32 [3072, 2, 1536], P('row', 'col'), may hold values from -0.00478416 to 0.00478416, as said below
Outputs:
- exchange: float32 [3072, 512], P(('row', 'col'))
The draws below stay inside these ranges and needn't reach their ends.
Inputs may be any that keep to these rules, and one draw needn't show every extreme that they name: V built from coulomb is symmetric.
All inputs are finite; a program needn't handle non-finite values.
Results may differ from the reference program's by a relative error of at most 0.0001.
Values sent between devices are 32-bit elements; how exact they have to be, the bound alone decides.
No kernel may reach another device: no remote copies, remote signals or barrier semaphores. Data moves between devices by JAX's collectives and lax.ppermute only.
A program may use at most 64 MiB of HBM per device.

```python
import jax
import jax.numpy as jnp
from jax import lax

NORB = 512
SH = 96
P_SIZE = 3072
N_ROW = 16
N_COL = 2


def draw_coulomb(key, part):
    full = jnp.clip(jax.random.normal(key, (P_SIZE, P_SIZE), jnp.float32), -4.0, 4.0)
    symmetric = (full + full.T) * 0.5 ** 0.5 * (P_SIZE * NORB) ** (-0.5)
    return symmetric.reshape(P_SIZE, N_ROW, N_COL, SH).transpose(0, 2, 1, 3).reshape(P_SIZE, N_COL, N_ROW * SH)


def block_scale(stream_key, extent, shards, low, top_value):
    def one(position, shards_of):
        steps = jax.random.uniform(jax.random.fold_in(jax.random.fold_in(stream_key, 6), position), (shards_of,), jnp.float32, low / len(shards), top_value / len(shards))
        return jnp.repeat(jnp.exp(steps), extent[position] // shards_of).reshape((-1,) + (1,) * (len(extent) - position - 1))

    loudness = one(*shards[0])
    for cut in shards[1:]:
        loudness = loudness * one(*cut)
    return loudness


def normal_values(own_key, dims, width, limit, split=(), held_as=jnp.bfloat16):
    loudness = block_scale(own_key, dims, split, -0.22, 0.18) if split else 1.0
    values = jax.random.normal(own_key, dims, jnp.float32) * width * loudness
    return jnp.minimum(jnp.maximum(values, -limit), limit).astype(held_as)


def setup_inputs(seed: int = 0) -> dict:
    splits = jax.random.split(jax.random.key(seed), 3)
    orbitals = normal_values(splits[0], (P_SIZE, NORB), 1.0, 6.0, ((0, 32),), jnp.float32)
    coulomb = draw_coulomb(jax.random.fold_in(splits[2], 71), 0)
    return dict(orbitals=orbitals, coulomb=coulomb)


def reference(orbitals, coulomb):
    matrix = coulomb.reshape(P_SIZE, N_COL, N_ROW, SH).transpose(0, 2, 1, 3).reshape(P_SIZE, P_SIZE)
    block_count = N_ROW
    orbit_blocks = orbitals.reshape(block_count, -1, NORB)
    coulomb_blocks = matrix.reshape(block_count, -1, P_SIZE)

    def one_block(pair):
        orbit_rows, coulomb_rows = pair
        gram_rows = jnp.dot(orbit_rows, orbitals.T, precision=lax.Precision.HIGHEST, preferred_element_type=jnp.float32)
        kernel_rows = gram_rows * coulomb_rows
        return jnp.dot(kernel_rows, orbitals, precision=lax.Precision.HIGHEST, preferred_element_type=jnp.float32)

    result = lax.map(one_block, (orbit_blocks, coulomb_blocks))
    return result.reshape(P_SIZE, NORB)
```

```python
import functools

import jax
import jax.numpy as jnp
from jax import lax
from jax.experimental import pallas as pl
from jax.experimental.pallas import tpu as pltpu
from jax.sharding import PartitionSpec as P

AXES = ("row", "col")
NT = (((1,), (1,)), ((), ()))
TN = (((0,), (0,)), ((), ()))


def split(x):
    high = x.astype(jnp.bfloat16)
    return high, (x - high.astype(jnp.float32)).astype(jnp.bfloat16)


def product(a, b, dims):
    dot = functools.partial(lax.dot_general, dimension_numbers=dims, preferred_element_type=jnp.float32)
    return dot(a[0], b[0]) + (dot(a[0], b[1]) + dot(a[1], b[0]))


def tile_kernel(n_panel, n_block, first, *refs):
    refs = list(refs)
    take = lambda n: [refs.pop(0) for _ in range(n)]
    (where,), panel, blocks, (kernel_t,) = take(1), take(n_panel), take(n_block), take(1)
    totals_in = [] if first else take(n_panel)
    totals = take(n_panel)
    points = blocks[0].shape[0]
    rows = split(jnp.concatenate([p[...] for p in panel], axis=0))
    columns = split(jnp.concatenate([b[...] for b in blocks], axis=0))
    coulomb = jnp.concatenate(
        [kernel_t[pl.ds(pl.multiple_of(where[i] * points, points), points), :] for i in range(n_block)], axis=0
    )
    tile = split(product(columns, rows, NT) * coulomb)
    result = product(tile, columns, TN)
    for i in range(n_panel):
        piece = result[i * points : (i + 1) * points]
        totals[i][...] = piece if first else totals_in[i][...] + piece


def add_tile(where, panel, blocks, kernel_t, totals):
    points, orbitals = blocks[0].shape
    n_panel, n_block, first = len(panel), len(blocks), totals is None
    rows, columns = n_panel * points, n_block * points
    operands = [where, *panel, *blocks, kernel_t] + ([] if first else list(totals))
    vmem = pl.BlockSpec(memory_space=pltpu.VMEM)
    return pl.pallas_call(
        functools.partial(tile_kernel, n_panel, n_block, first),
        out_shape=[jax.ShapeDtypeStruct((points, orbitals), jnp.float32)] * n_panel,
        in_specs=[pl.BlockSpec(memory_space=pltpu.SMEM)] + [vmem] * (len(operands) - 1),
        out_specs=[vmem] * n_panel,
        cost_estimate=pl.CostEstimate(
            flops=12 * rows * columns * orbitals, bytes_accessed=4 * (rows + columns) * orbitals, transcendentals=0
        ),
        compiler_params=pltpu.CompilerParams(vmem_limit_bytes=24 << 20),
        name="add_tile",
    )(*operands)


def solution(mesh):
    n_row, n_col = mesh.shape["row"], mesh.shape["col"]

    def move(x, target):
        pairs = []
        for r in range(n_row):
            for c in range(n_col):
                r2, c2 = target(r, c)
                pairs.append((r * n_col + c, r2 * n_col + c2))
        return lax.ppermute(x, AXES, pairs)

    def hop(x, even, odd):
        return move(x, lambda r, c: (r ^ (odd if c % 2 else even), c))

    def turn(x, k):
        return move(x, lambda r, c: (r, (c + k) % n_col))

    def body(orbitals, coulomb):
        row, col = lax.axis_index("row"), lax.axis_index("col")
        points = orbitals.shape[0]
        panel = [orbitals] + [turn(orbitals, -k) for k in range(1, n_col)]
        tile = coulomb.reshape(n_col * points, n_row * points)
        kernel_t = jnp.concatenate(
            [lax.dynamic_slice_in_dim(tile, (col + k) % n_col * points, points, 0).T for k in range(n_col)], axis=1
        )
        odd = col % 2
        first_step, second_step = 1 + odd, 2 - odd
        totals = None
        slots = [(orbitals, 0)] + [(hop(orbitals, far, far), far) for far in range(4, n_row, 4)]
        for block, far in slots:
            first = hop(block, 1, 2)
            second = hop(block, 2, 1)
            third = hop(first, 2, 1)
            base = row ^ far
            where = jnp.stack([base, base ^ first_step, base ^ second_step, base ^ 3]).astype(jnp.int32)
            totals = add_tile(where, panel, [block, first, second, third], kernel_t, totals)
        result = totals[0]
        for k in range(1, n_col):
            result = result + turn(totals[k], k)
        return result

    placed = (P(("row", "col"), None), P("row", "col", None))
    return jax.shard_map(body, mesh=mesh, in_specs=placed, out_specs=P(("row", "col"), None), check_vma=False)
```
